128 devices in a mesh: rows: 128 (over y, x, z, core).
Axes of the slice: x: 4, y: 4, z: 4, core: 2. Of those that a mesh axis runs over, the one named last changes fastest.
Arguments:
- tracers_init: float32 [65536, 256], P('rows'), may hold values from -6 to 6
- source: float32 [65536, 256], P('rows'), may hold values from -4 to 4
- explicit_tiles: float32 [512, 8, 128, 128], P('rows'), may hold values from -0.0625 to 0.0625
- implicit_tiles: float32 [512, 8, 128, 128], P('rows'), may hold values from -0.0625 to 0.0625
- explicit_cols: int32 [512, 8], P('rows'), may hold values from 0 to 6, as said below
- implicit_cols: int32 [512, 8], P('rows'), may hold values from 0 to 6, as said below
- send_rows: int32 [1024, 48], P('rows'), may hold values from 0 to 511
Outputs:
- tracers: float32 [65536, 256], P('rows')
The draws below stay inside these ranges and needn't reach their ends.
Inputs may be any that keep to these rules, and one draw needn't show every extreme that they name: `explicit_cols`: each entry names one of the 7 blocks of the device's own rows followed by its halo rows. `implicit_cols`: each entry names one of the 7 blocks of the device's own rows followed by its halo rows. `send_rows`: local row numbers of the sending device.
All inputs are finite; a program needn't handle non-finite values.
Results may differ from the reference program's by a relative error of at most 0.0001.
Values sent between devices are 32-bit elements; how exact they have to be, the bound alone decides.
A program may use at most 64 MiB of HBM per device.

```python
import jax
import jax.numpy as jnp
from jax import lax

P_SIZE = 256
B = 128
K = 8
NEAR = 4
H = 48
STEPS = 3
NB_DEV = 4
TOTAL_BLK = 512
ROWS = 65536
TOTAL_OFF = 1024
EXT_BLK = 7
N_ROWS = 128


def column_pattern(key, salt):
    folded = jax.random.fold_in(key, salt)
    halo_blocks = EXT_BLK - NB_DEV
    columns = jax.random.randint(folded, (TOTAL_BLK, K), 0, EXT_BLK)
    within = jnp.arange(TOTAL_BLK, dtype=jnp.int32) % NB_DEV
    halo_pick = NB_DEV + within % halo_blocks
    first = jnp.where(within < 2 * halo_blocks, halo_pick, columns[:, 0])
    columns = columns.at[:, 0].set(first)
    columns = columns.at[:, 1].set(within)
    return columns.astype(jnp.int32)


def draw_explicit_cols(key, part):
    return column_pattern(key, 11)


def draw_implicit_cols(key, part):
    return column_pattern(key, 23)


def set_ends(values, rng, least, largest):
    index_at = [jax.random.randint(jax.random.fold_in(rng, axis), (), 0, length) for axis, length in enumerate(values.shape)]
    widest = values.shape.index(max(values.shape))
    neighbour = index_at[:widest] + [(index_at[widest] + 1) % values.shape[widest]] + index_at[widest + 1:]
    return values.at[tuple(index_at)].set(least).at[tuple(neighbour)].set(largest)


def levels(own_key, shape, cuts, smallest, largest):
    level = 1.0
    for position, blocks in cuts:
        steps = jax.random.uniform(jax.random.fold_in(jax.random.fold_in(own_key, 6), position), (blocks,), jnp.float32, smallest / len(cuts), largest / len(cuts))
        level = level * jnp.repeat(jnp.exp(steps), shape[position] // blocks).reshape((-1,) + (1,) * (len(shape) - 1 - position))
    return level


def bell_draw(rng, extent, width, limit, cuts=(), held_as=jnp.bfloat16):
    entries = width * jax.random.normal(rng, extent, jnp.float32)
    if cuts:
        entries = entries * levels(rng, extent, cuts, -0.22, 0.18)
    return jnp.clip(entries, -limit, limit).astype(held_as)


def setup_inputs(seed: int = 0) -> dict:
    keys = jax.random.split(jax.random.key(seed), 8)
    return {
        "tracers_init": bell_draw(keys[0], (ROWS, P_SIZE), 1.0, 6.0, ((0, 128),), jnp.float32),
        "source": bell_draw(keys[1], (ROWS, P_SIZE), 0.5, 4.0, ((0, 128),), jnp.float32),
        "explicit_tiles": bell_draw(keys[2], (TOTAL_BLK, K, B, B), (8 * K * B) ** -0.5, 0.0625, ((0, 128),), jnp.float32),
        "implicit_tiles": bell_draw(keys[3], (TOTAL_BLK, K, B, B), (8 * K * B) ** -0.5, 0.0625, ((0, 128),), jnp.float32),
        "explicit_cols": draw_explicit_cols(jax.random.fold_in(keys[7], 71), 0),
        "implicit_cols": draw_implicit_cols(jax.random.fold_in(keys[7], 71), 0),
        "send_rows": set_ends(jax.random.randint(keys[6], (TOTAL_OFF, H), 0, NB_DEV * B), jax.random.fold_in(keys[6], 1), 0, (NB_DEV * B) - 1).astype(jnp.int32),
    }


def partner_offset(offset_index):
    return (offset_index // 2 + 1) * (1 if offset_index % 2 == 0 else -1)


def local_apply(tiles, columns, own_rows, halo_rows):
    extended = jnp.concatenate([own_rows, halo_rows], axis=0).reshape(EXT_BLK, B, P_SIZE)
    total = own_rows.reshape(NB_DEV, B, P_SIZE)
    for slot_index in range(K):
        picked = extended[columns[:, slot_index]]
        total = total + jnp.einsum("rij,rjp->rip", tiles[:, slot_index], picked, precision=lax.Precision.HIGHEST)
    return total.reshape(NB_DEV * B, P_SIZE)


def reference(tracers_init, source, explicit_tiles, implicit_tiles, explicit_cols, implicit_cols, send_rows):
    sends = send_rows.reshape(N_ROWS, 2 * NEAR, H)

    def halo_all(state):
        owned = state.reshape(N_ROWS, NB_DEV * B, P_SIZE)
        payloads = jax.vmap(lambda rows_of, lists: rows_of[lists])(owned, sends)
        pieces = [jnp.roll(payloads[:, offset_index], partner_offset(offset_index), axis=0) for offset_index in range(2 * NEAR)]
        return jnp.concatenate(pieces, axis=1)

    def apply(tiles, columns, state):
        halo = halo_all(state)
        owned = state.reshape(N_ROWS, NB_DEV * B, P_SIZE)
        tiles_dev = tiles.reshape(N_ROWS, NB_DEV, K, B, B)
        columns_dev = columns.reshape(N_ROWS, NB_DEV, K)
        result = lax.map(lambda parts: local_apply(parts[0], parts[1], parts[2], parts[3]), (tiles_dev, columns_dev, owned, halo))
        return result.reshape(N_ROWS * NB_DEV * B, P_SIZE)

    tracers = tracers_init
    for repeat in range(STEPS):
        middle = apply(explicit_tiles, explicit_cols, tracers) + source
        tracers = apply(implicit_tiles, implicit_cols, middle)
    return tracers
```

```python
import functools

import jax
import jax.numpy as jnp
from jax import lax
from jax.experimental import pallas as pl
from jax.experimental.pallas import tpu as pltpu
from jax.sharding import PartitionSpec as P

STEPS = 3
LANES = 128
MESH = pl.DeviceIdType.MESH
F32 = jnp.float32
BF16 = jnp.bfloat16


def partner_offset(offset_index):
    return (offset_index // 2 + 1) * (1 if offset_index % 2 == 0 else -1)


def split2(x):
    hi = x.astype(BF16)
    lo = (x - hi.astype(F32)).astype(BF16)
    return hi, lo


def dot(a, b):
    return jnp.dot(a, b, preferred_element_type=F32)


def product(w_hi, w_lo, cat):
    wide = dot(w_hi, cat)
    return (wide[:, :LANES] + wide[:, LANES:]) + dot(w_lo, cat[:, :LANES])


def kernel(
    devices,
    v0_hbm,
    src_hbm,
    et_hbm,
    it_hbm,
    ec_hbm,
    ic_hbm,
    send_hbm,
    out_ref,
    v0,
    src,
    tiles,
    cols,
    send_v,
    square,
    pick,
    w_hi,
    w_lo,
    pay,
    halo,
    vcat,
    vpart,
    part,
    psrc,
    load_sem,
    send_sem,
    recv_sem,
):
    partners, per_list = send_v.shape
    own = v0.shape[0]
    listed = partners * per_list
    blocks, slots, size, _ = et_hbm.shape
    ext_blocks = (own + listed) // size
    halves = v0.shape[1] // LANES
    exchanges = 2 * STEPS

    me = lax.axis_index("rows")
    targets = [lax.rem(me + partner_offset(o) + devices, devices) for o in range(partners)]

    barrier = pltpu.get_barrier_semaphore()
    for target in targets:
        pl.semaphore_signal(barrier, inc=1, device_id=(target,), device_id_type=MESH)

    loads = [
        pltpu.make_async_copy(send_hbm, send_v, load_sem.at[0]),
        pltpu.make_async_copy(v0_hbm, v0, load_sem.at[1]),
        pltpu.make_async_copy(et_hbm, tiles.at[0], load_sem.at[2]),
        pltpu.make_async_copy(ec_hbm, cols.at[0], load_sem.at[3]),
        pltpu.make_async_copy(src_hbm, src, load_sem.at[4]),
        pltpu.make_async_copy(it_hbm, tiles.at[1], load_sem.at[5]),
        pltpu.make_async_copy(ic_hbm, cols.at[1], load_sem.at[6]),
    ]
    for load in loads:
        load.start()

    def copies(exchange, half):
        order = sorted(range(partners), key=lambda o: -abs(partner_offset(o)))
        return [
            pltpu.make_async_remote_copy(
                src_ref=pay.at[exchange, half, pl.ds(o * per_list, per_list)],
                dst_ref=halo.at[exchange, half, pl.ds(o * per_list, per_list)],
                send_sem=send_sem.at[exchange, half, o],
                recv_sem=recv_sem.at[exchange, half, o],
                device_id=(targets[o],),
                device_id_type=MESH,
            )
            for o in order
        ]

    square[...] = jnp.zeros_like(square)
    loads[0].wait()
    square[0:partners, 0:per_list] = send_v[...].astype(F32)
    turned = square[...].T
    lane = lax.broadcasted_iota(jnp.int32, (per_list, LANES), 1).astype(F32)
    for o in range(partners):
        column = jnp.broadcast_to(turned[0:per_list, o : o + 1], (per_list, LANES))
        for c in range(own // LANES):
            pick[o * per_list : (o + 1) * per_list, c * LANES : (c + 1) * LANES] = jnp.where(
                column == lane + float(c * LANES), 1.0, 0.0
            ).astype(BF16)

    def picked(x):
        hi, mid = split2(x)
        low = ((x - hi.astype(F32)) - mid.astype(F32)).astype(BF16)
        wide = dot(pick[...], jnp.concatenate([hi, mid], axis=1))
        return (wide[:, :LANES] + wide[:, LANES:]) + dot(pick[...], low)

    loads[1].wait()
    for half in range(halves):
        pay[0, half] = picked(v0[:, half * LANES : (half + 1) * LANES])
        if half == 0:
            pl.semaphore_wait(barrier, partners)
        for copy in copies(0, half):
            copy.start()

    def build(which):
        for g in range(blocks):
            named = [cols[which, g, k] for k in range(slots)]
            for c in range(ext_blocks):
                total = None
                for k in range(slots):
                    term = tiles[which, g, k] * jnp.where(named[k] == c, 1.0, 0.0).astype(F32)
                    total = term if total is None else total + term
                hi, lo = split2(total)
                rows = slice(listed + g * size, listed + (g + 1) * size)
                w_hi[which, rows, c * size : (c + 1) * size] = hi
                w_lo[which, rows, c * size : (c + 1) * size] = lo
        for w in (w_hi, w_lo):
            w[which, 0:listed] = dot(pick[...], w[which, listed:]).astype(BF16)

    loads[2].wait()
    loads[3].wait()
    build(0)
    loads[4].wait()
    for half in range(halves):
        psrc[half] = picked(src[:, half * LANES : (half + 1) * LANES])

    def own_part(which, half, state, payload, with_source):
        hi, lo = split2(state)
        vcat[half, :, 0:LANES] = hi
        vcat[half, :, LANES:] = lo
        near = product(w_hi[which, :, 0:own], w_lo[which, :, 0:own], vcat[half])
        head, body = payload + near[0:listed], state + near[listed:]
        if with_source:
            head = head + psrc[half]
            body = body + src[:, half * LANES : (half + 1) * LANES]
        part[half] = head
        vpart[half] = body

    for half in range(halves):
        own_part(0, half, v0[:, half * LANES : (half + 1) * LANES], pay[0, half], True)
    loads[5].wait()
    loads[6].wait()
    build(1)

    def stage(exchange, which, half, last):
        for copy in copies(exchange, half):
            copy.wait_recv()
        hi, lo = split2(halo[exchange, half])
        hcat = jnp.concatenate([hi, lo], axis=1)
        if not last:
            payload = part[half] + product(
                w_hi[which, 0:listed, own:], w_lo[which, 0:listed, own:], hcat
            )
            pay[exchange + 1, half] = payload
            for copy in copies(exchange + 1, half):
                copy.start()
        state = vpart[half] + product(
            w_hi[which, listed:, own:], w_lo[which, listed:, own:], hcat
        )
        if last:
            out_ref[:, half * LANES : (half + 1) * LANES] = state
        else:
            own_part(1 - which, half, state, pay[exchange + 1, half], which == 1)

    for exchange in range(exchanges):
        for half in range(halves):
            stage(exchange, exchange % 2, half, exchange == exchanges - 1)

    for exchange in range(exchanges):
        for half in range(halves):
            for copy in copies(exchange, half):
                copy.wait_send()


def on_device(devices, v0, source, et, it, ec, ic, send):
    own, panels = v0.shape
    partners, per_list = send.shape
    blocks, slots, size, _ = et.shape
    listed = partners * per_list
    extended = own + listed
    halves = panels // LANES
    exchanges = 2 * STEPS
    any_spec = pl.BlockSpec(memory_space=pl.ANY)
    return pl.pallas_call(
        functools.partial(kernel, devices),
        out_shape=jax.ShapeDtypeStruct((own, panels), F32),
        in_specs=[any_spec] * 7,
        out_specs=pl.BlockSpec(memory_space=pltpu.VMEM),
        scratch_shapes=[
            pltpu.VMEM((own, panels), F32),
            pltpu.VMEM((own, panels), F32),
            pltpu.VMEM((2, blocks, slots, size, size), F32),
            pltpu.SMEM((2, blocks, slots), jnp.int32),
            pltpu.VMEM((partners, per_list), jnp.int32),
            pltpu.VMEM((LANES, LANES), F32),
            pltpu.VMEM((listed, own), BF16),
            pltpu.VMEM((2, extended, extended), BF16),
            pltpu.VMEM((2, extended, extended), BF16),
            pltpu.VMEM((exchanges, halves, listed, LANES), F32),
            pltpu.VMEM((exchanges, halves, listed, LANES), F32),
            pltpu.VMEM((halves, own, 2 * LANES), BF16),
            pltpu.VMEM((halves, own, LANES), F32),
            pltpu.VMEM((halves, listed, LANES), F32),
            pltpu.VMEM((halves, listed, LANES), F32),
            pltpu.SemaphoreType.DMA((7,)),
            pltpu.SemaphoreType.DMA((exchanges, halves, partners)),
            pltpu.SemaphoreType.DMA((exchanges, halves, partners)),
        ],
        compiler_params=pltpu.CompilerParams(
            collective_id=0, has_side_effects=True, vmem_limit_bytes=48 * 1024 * 1024
        ),
    )(v0, source, et, it, ec, ic, send)


def solution(mesh):
    return jax.shard_map(
        functools.partial(on_device, mesh.shape["rows"]),
        mesh=mesh,
        in_specs=(
            P("rows", None),
            P("rows", None),
            P("rows", None, None, None),
            P("rows", None, None, None),
            P("rows", None),
            P("rows", None),
            P("rows", None),
        ),
        out_specs=P("rows", None),
        check_vma=False,
    )
```

```python
import functools

import jax
import jax.numpy as jnp
from jax import lax
from jax.experimental import pallas as pl
from jax.experimental.pallas import tpu as pltpu
from jax.sharding import PartitionSpec as P

STEPS = 3
LANES = 128
MESH = pl.DeviceIdType.MESH
F32 = jnp.float32
BF16 = jnp.bfloat16


def partner_offset(offset_index):
    return (offset_index // 2 + 1) * (1 if offset_index % 2 == 0 else -1)


def split2(x):
    hi = x.astype(BF16)
    lo = (x - hi.astype(F32)).astype(BF16)
    return hi, lo


def dot(a, b):
    return jnp.dot(a, b, preferred_element_type=F32)


def product(w_hi, w_lo, cat):
    wide = dot(w_hi, cat)
    return (wide[:, :LANES] + wide[:, LANES:]) + dot(w_lo, cat[:, :LANES])


def kernel(
    devices,
    v0_hbm,
    src_hbm,
    et_hbm,
    it_hbm,
    ec_hbm,
    ic_hbm,
    send_hbm,
    out_ref,
    v0,
    src,
    tiles,
    cols,
    send_v,
    square,
    pick,
    w_hi,
    w_lo,
    pay,
    halo,
    vcat,
    vpart,
    part,
    psrc,
    load_sem,
    send_sem,
    recv_sem,
):
    partners, per_list = send_v.shape
    own = v0.shape[0]
    listed = partners * per_list
    blocks, slots, size, _ = et_hbm.shape
    ext_blocks = (own + listed) // size
    halves = v0.shape[1] // LANES
    exchanges = 2 * STEPS

    me = lax.axis_index("rows")
    targets = [lax.rem(me + partner_offset(o) + devices, devices) for o in range(partners)]

    barrier = pltpu.get_barrier_semaphore()
    for target in targets:
        pl.semaphore_signal(barrier, inc=1, device_id=(target,), device_id_type=MESH)

    loads = [
        pltpu.make_async_copy(send_hbm, send_v, load_sem.at[0]),
        pltpu.make_async_copy(v0_hbm, v0, load_sem.at[1]),
        pltpu.make_async_copy(et_hbm, tiles.at[0], load_sem.at[2]),
        pltpu.make_async_copy(ec_hbm, cols.at[0], load_sem.at[3]),
        pltpu.make_async_copy(src_hbm, src, load_sem.at[4]),
        pltpu.make_async_copy(it_hbm, tiles.at[1], load_sem.at[5]),
        pltpu.make_async_copy(ic_hbm, cols.at[1], load_sem.at[6]),
    ]
    for load in loads:
        load.start()

    def copies(exchange, half):
        order = sorted(range(partners), key=lambda o: -abs(partner_offset(o)))
        return [
            pltpu.make_async_remote_copy(
                src_ref=pay.at[exchange, half, pl.ds(o * per_list, per_list)],
                dst_ref=halo.at[exchange, half, pl.ds(o * per_list, per_list)],
                send_sem=send_sem.at[exchange, half, o],
                recv_sem=recv_sem.at[exchange, half, o],
                device_id=(targets[o],),
                device_id_type=MESH,
            )
            for o in order
        ]

    square[...] = jnp.zeros_like(square)
    loads[0].wait()
    square[0:partners, 0:per_list] = send_v[...].astype(F32)
    turned = square[...].T
    lane = lax.broadcasted_iota(jnp.int32, (per_list, LANES), 1).astype(F32)
    for o in range(partners):
        column = jnp.broadcast_to(turned[0:per_list, o : o + 1], (per_list, LANES))
        for c in range(own // LANES):
            pick[o * per_list : (o + 1) * per_list, c * LANES : (c + 1) * LANES] = jnp.where(
                column == lane + float(c * LANES), 1.0, 0.0
            ).astype(BF16)

    def picked(x):
        hi, mid = split2(x)
        low = ((x - hi.astype(F32)) - mid.astype(F32)).astype(BF16)
        wide = dot(pick[...], jnp.concatenate([hi, mid], axis=1))
        return (wide[:, :LANES] + wide[:, LANES:]) + dot(pick[...], low)

    loads[1].wait()
    for half in range(halves):
        pay[0, half] = picked(v0[:, half * LANES : (half + 1) * LANES])
        if half == 0:
            pl.semaphore_wait(barrier, partners)
        for copy in copies(0, half):
            copy.start()

    def build(which):
        for g in range(blocks):
            named = [cols[which, g, k] for k in range(slots)]
            for c in range(ext_blocks):
                total = None
                for k in range(slots):
                    term = tiles[which, g, k] * jnp.where(named[k] == c, 1.0, 0.0).astype(F32)
                    total = term if total is None else total + term
                hi, lo = split2(total)
                rows = slice(listed + g * size, listed + (g + 1) * size)
                w_hi[which, rows, c * size : (c + 1) * size] = hi
                w_lo[which, rows, c * size : (c + 1) * size] = lo
        for w in (w_hi, w_lo):
            w[which, 0:listed] = dot(pick[...], w[which, listed:]).astype(BF16)

    loads[2].wait()
    loads[3].wait()
    build(0)
    loads[4].wait()
    for half in range(halves):
        psrc[half] = picked(src[:, half * LANES : (half + 1) * LANES])

    def own_part(which, half, state, payload, with_source):
        hi, lo = split2(state)
        vcat[half, :, 0:LANES] = hi
        vcat[half, :, LANES:] = lo
        near = product(w_hi[which, :, 0:own], w_lo[which, :, 0:own], vcat[half])
        head, body = payload + near[0:listed], state + near[listed:]
        if with_source:
            head = head + psrc[half]
            body = body + src[:, half * LANES : (half + 1) * LANES]
        part[half] = head
        vpart[half] = body

    for half in range(halves):
        own_part(0, half, v0[:, half * LANES : (half + 1) * LANES], pay[0, half], True)
    loads[5].wait()
    loads[6].wait()
    build(1)

    def stage(exchange, which, half, last):
        for copy in copies(exchange, half):
            copy.wait_recv()
        hi, lo = split2(halo[exchange, half])
        hcat = jnp.concatenate([hi, lo], axis=1)
        if not last:
            payload = part[half] + product(
                w_hi[which, 0:listed, own:], w_lo[which, 0:listed, own:], hcat
            )
            pay[exchange + 1, half] = payload
            for copy in copies(exchange + 1, half):
                copy.start()
        state = vpart[half] + product(
            w_hi[which, listed:, own:], w_lo[which, listed:, own:], hcat
        )
        if last:
            out_ref[:, half * LANES : (half + 1) * LANES] = state
        else:
            own_part(1 - which, half, state, pay[exchange + 1, half], which == 1)

    for exchange in range(exchanges):
        for half in range(halves):
            stage(exchange, exchange % 2, half, exchange == exchanges - 1)

    for exchange in range(exchanges):
        for half in range(halves):
            for copy in copies(exchange, half):
                copy.wait_send()


def on_device(devices, v0, source, et, it, ec, ic, send):
    own, panels = v0.shape
    partners, per_list = send.shape
    blocks, slots, size, _ = et.shape
    listed = partners * per_list
    extended = own + listed
    halves = panels // LANES
    exchanges = 2 * STEPS
    in_hbm = pl.BlockSpec(memory_space=pltpu.HBM)
    return pl.pallas_call(
        functools.partial(kernel, devices),
        out_shape=jax.ShapeDtypeStruct((own, panels), F32),
        in_specs=[in_hbm] * 7,
        out_specs=pl.BlockSpec(memory_space=pltpu.VMEM),
        scratch_shapes=[
            pltpu.VMEM((own, panels), F32),
            pltpu.VMEM((own, panels), F32),
            pltpu.VMEM((2, blocks, slots, size, size), F32),
            pltpu.SMEM((2, blocks, slots), jnp.int32),
            pltpu.VMEM((partners, per_list), jnp.int32),
            pltpu.VMEM((LANES, LANES), F32),
            pltpu.VMEM((listed, own), BF16),
            pltpu.VMEM((2, extended, extended), BF16),
            pltpu.VMEM((2, extended, extended), BF16),
            pltpu.VMEM((exchanges, halves, listed, LANES), F32),
            pltpu.VMEM((exchanges, halves, listed, LANES), F32),
            pltpu.VMEM((halves, own, 2 * LANES), BF16),
            pltpu.VMEM((halves, own, LANES), F32),
            pltpu.VMEM((halves, listed, LANES), F32),
            pltpu.VMEM((halves, listed, LANES), F32),
            pltpu.SemaphoreType.DMA((7,)),
            pltpu.SemaphoreType.DMA((exchanges, halves, partners)),
            pltpu.SemaphoreType.DMA((exchanges, halves, partners)),
        ],
        compiler_params=pltpu.CompilerParams(
            collective_id=0, has_side_effects=True, vmem_limit_bytes=48 * 1024 * 1024
        ),
    )(
        *[
            pltpu.with_memory_space_constraint(x, pltpu.HBM)
            for x in (v0, source, et, it, ec, ic, send)
        ]
    )


def solution(mesh):
    return jax.shard_map(
        functools.partial(on_device, mesh.shape["rows"]),
        mesh=mesh,
        in_specs=(
            P("rows", None),
            P("rows", None),
            P("rows", None, None, None),
            P("rows", None, None, None),
            P("rows", None),
            P("rows", None),
            P("rows", None),
        ),
        out_specs=P("rows", None),
        check_vma=False,
    )
```

```python
import functools

import jax
import jax.numpy as jnp
from jax import lax
from jax.experimental import pallas as pl
from jax.experimental.pallas import tpu as pltpu
from jax.sharding import PartitionSpec as P

STEPS = 3
LANES = 128
MESH = pl.DeviceIdType.MESH
F32 = jnp.float32
BF16 = jnp.bfloat16


def partner_offset(offset_index):
    return (offset_index // 2 + 1) * (1 if offset_index % 2 == 0 else -1)


def split2(x):
    hi = x.astype(BF16)
    lo = (x - hi.astype(F32)).astype(BF16)
    return hi, lo


def dot(a, b):
    return jnp.dot(a, b, preferred_element_type=F32)


def product(w_hi, w_lo, cat):
    wide = dot(w_hi, cat)
    return (wide[:, :LANES] + wide[:, LANES:]) + dot(w_lo, cat[:, :LANES])


def kernel(
    devices,
    v0_hbm,
    src_hbm,
    et_hbm,
    it_hbm,
    ec_hbm,
    ic_hbm,
    send_hbm,
    out_ref,
    v0,
    src,
    tiles,
    cols,
    send_v,
    square,
    pick,
    w_hi,
    w_lo,
    pay,
    halo,
    vcat,
    vpart,
    part,
    psrc,
    load_sem,
    send_sem,
    recv_sem,
):
    partners, per_list = send_v.shape
    own = v0.shape[0]
    listed = partners * per_list
    blocks, slots, size, _ = et_hbm.shape
    ext_blocks = (own + listed) // size
    halves = v0.shape[1] // LANES
    exchanges = 2 * STEPS

    me = lax.axis_index("rows")
    targets = [lax.rem(me + partner_offset(o) + devices, devices) for o in range(partners)]

    barrier = pltpu.get_barrier_semaphore()
    for target in targets:
        pl.semaphore_signal(barrier, inc=1, device_id=(target,), device_id_type=MESH)

    loads = [
        pltpu.make_async_copy(send_hbm, send_v, load_sem.at[0]),
        pltpu.make_async_copy(v0_hbm, v0, load_sem.at[1]),
        pltpu.make_async_copy(et_hbm, tiles.at[0], load_sem.at[2]),
        pltpu.make_async_copy(ec_hbm, cols.at[0], load_sem.at[3]),
        pltpu.make_async_copy(src_hbm, src, load_sem.at[4]),
        pltpu.make_async_copy(it_hbm, tiles.at[1], load_sem.at[5]),
        pltpu.make_async_copy(ic_hbm, cols.at[1], load_sem.at[6]),
    ]
    for load in loads:
        load.start()

    def copies(exchange, half):
        return [
            pltpu.make_async_remote_copy(
                src_ref=pay.at[exchange, half, pl.ds(o * per_list, per_list)],
                dst_ref=halo.at[exchange, half, pl.ds(o * per_list, per_list)],
                send_sem=send_sem.at[exchange, half, o],
                recv_sem=recv_sem.at[exchange, half, o],
                device_id=(targets[o],),
                device_id_type=MESH,
            )
            for o in range(partners)
        ]

    def send(exchange, half):
        ready = copies(exchange, half)
        near = sorted(range(partners), key=lambda o: abs(partner_offset(o)))
        for core in range(2):
            order = sorted(near, key=lambda o: (partner_offset(o) + core) % 2)

            @pl.when(lax.rem(me, 2) == core)
            def _():
                for o in order:
                    ready[o].start()

    square[...] = jnp.zeros_like(square)
    loads[0].wait()
    square[0:partners, 0:per_list] = send_v[...].astype(F32)
    turned = square[...].T
    lane = lax.broadcasted_iota(jnp.int32, (per_list, LANES), 1).astype(F32)
    for o in range(partners):
        column = jnp.broadcast_to(turned[0:per_list, o : o + 1], (per_list, LANES))
        for c in range(own // LANES):
            pick[o * per_list : (o + 1) * per_list, c * LANES : (c + 1) * LANES] = jnp.where(
                column == lane + float(c * LANES), 1.0, 0.0
            ).astype(BF16)

    def picked(x):
        hi, mid = split2(x)
        low = ((x - hi.astype(F32)) - mid.astype(F32)).astype(BF16)
        wide = dot(pick[...], jnp.concatenate([hi, mid], axis=1))
        return (wide[:, :LANES] + wide[:, LANES:]) + dot(pick[...], low)

    loads[1].wait()
    for half in range(halves):
        pay[0, half] = picked(v0[:, half * LANES : (half + 1) * LANES])
        if half == 0:
            pl.semaphore_wait(barrier, partners)
        send(0, half)

    def build(which):
        for g in range(blocks):
            named = [cols[which, g, k] for k in range(slots)]
            for c in range(ext_blocks):
                total = None
                for k in range(slots):
                    term = tiles[which, g, k] * jnp.where(named[k] == c, 1.0, 0.0).astype(F32)
                    total = term if total is None else total + term
                hi, lo = split2(total)
                rows = slice(listed + g * size, listed + (g + 1) * size)
                w_hi[which, rows, c * size : (c + 1) * size] = hi
                w_lo[which, rows, c * size : (c + 1) * size] = lo
        for w in (w_hi, w_lo):
            w[which, 0:listed] = dot(pick[...], w[which, listed:]).astype(BF16)

    loads[2].wait()
    loads[3].wait()
    build(0)
    loads[4].wait()
    for half in range(halves):
        psrc[half] = picked(src[:, half * LANES : (half + 1) * LANES])

    def own_part(which, half, state, payload, with_source):
        hi, lo = split2(state)
        vcat[half, :, 0:LANES] = hi
        vcat[half, :, LANES:] = lo
        near = product(w_hi[which, :, 0:own], w_lo[which, :, 0:own], vcat[half])
        head, body = payload + near[0:listed], state + near[listed:]
        if with_source:
            head = head + psrc[half]
            body = body + src[:, half * LANES : (half + 1) * LANES]
        part[half] = head
        vpart[half] = body

    for half in range(halves):
        own_part(0, half, v0[:, half * LANES : (half + 1) * LANES], pay[0, half], True)
    loads[5].wait()
    loads[6].wait()
    build(1)

    def stage(exchange, which, half, last):
        for copy in copies(exchange, half):
            copy.wait_recv()
        hi, lo = split2(halo[exchange, half])
        hcat = jnp.concatenate([hi, lo], axis=1)
        if not last:
            payload = part[half] + product(
                w_hi[which, 0:listed, own:], w_lo[which, 0:listed, own:], hcat
            )
            pay[exchange + 1, half] = payload
            send(exchange + 1, half)
        state = vpart[half] + product(
            w_hi[which, listed:, own:], w_lo[which, listed:, own:], hcat
        )
        if last:
            out_ref[:, half * LANES : (half + 1) * LANES] = state
        else:
            own_part(1 - which, half, state, pay[exchange + 1, half], which == 1)

    for exchange in range(exchanges):
        for half in range(halves):
            stage(exchange, exchange % 2, half, exchange == exchanges - 1)

    for exchange in range(exchanges):
        for half in range(halves):
            for copy in copies(exchange, half):
                copy.wait_send()


def on_device(devices, v0, source, et, it, ec, ic, send):
    own, panels = v0.shape
    partners, per_list = send.shape
    blocks, slots, size, _ = et.shape
    listed = partners * per_list
    extended = own + listed
    halves = panels // LANES
    exchanges = 2 * STEPS
    in_hbm = pl.BlockSpec(memory_space=pltpu.HBM)
    return pl.pallas_call(
        functools.partial(kernel, devices),
        out_shape=jax.ShapeDtypeStruct((own, panels), F32),
        in_specs=[in_hbm] * 7,
        out_specs=pl.BlockSpec(memory_space=pltpu.VMEM),
        scratch_shapes=[
            pltpu.VMEM((own, panels), F32),
            pltpu.VMEM((own, panels), F32),
            pltpu.VMEM((2, blocks, slots, size, size), F32),
            pltpu.SMEM((2, blocks, slots), jnp.int32),
            pltpu.VMEM((partners, per_list), jnp.int32),
            pltpu.VMEM((LANES, LANES), F32),
            pltpu.VMEM((listed, own), BF16),
            pltpu.VMEM((2, extended, extended), BF16),
            pltpu.VMEM((2, extended, extended), BF16),
            pltpu.VMEM((exchanges, halves, listed, LANES), F32),
            pltpu.VMEM((exchanges, halves, listed, LANES), F32),
            pltpu.VMEM((halves, own, 2 * LANES), BF16),
            pltpu.VMEM((halves, own, LANES), F32),
            pltpu.VMEM((halves, listed, LANES), F32),
            pltpu.VMEM((halves, listed, LANES), F32),
            pltpu.SemaphoreType.DMA((7,)),
            pltpu.SemaphoreType.DMA((exchanges, halves, partners)),
            pltpu.SemaphoreType.DMA((exchanges, halves, partners)),
        ],
        compiler_params=pltpu.CompilerParams(
            collective_id=0, has_side_effects=True, vmem_limit_bytes=48 * 1024 * 1024
        ),
    )(
        *[
            pltpu.with_memory_space_constraint(x, pltpu.HBM)
            for x in (v0, source, et, it, ec, ic, send)
        ]
    )


def solution(mesh):
    return jax.shard_map(
        functools.partial(on_device, mesh.shape["rows"]),
        mesh=mesh,
        in_specs=(
            P("rows", None),
            P("rows", None),
            P("rows", None, None, None),
            P("rows", None, None, None),
            P("rows", None),
            P("rows", None),
            P("rows", None),
        ),
        out_specs=P("rows", None),
        check_vma=False,
    )
```

```python
import functools

import jax
import jax.numpy as jnp
from jax import lax
from jax.experimental import pallas as pl
from jax.experimental.pallas import tpu as pltpu
from jax.sharding import PartitionSpec as P

STEPS = 3
LANES = 128
MESH = pl.DeviceIdType.MESH
F32 = jnp.float32
BF16 = jnp.bfloat16


def partner_offset(offset_index):
    return (offset_index // 2 + 1) * (1 if offset_index % 2 == 0 else -1)


def split2(x):
    hi = x.astype(BF16)
    lo = (x - hi.astype(F32)).astype(BF16)
    return hi, lo


def dot(a, b):
    return jnp.dot(a, b, preferred_element_type=F32)


def product(w_hi, w_lo, cat):
    wide = dot(w_hi, cat)
    return (wide[:, :LANES] + wide[:, LANES:]) + dot(w_lo, cat[:, :LANES])


def kernel(
    devices,
    v0_hbm,
    src_hbm,
    et_hbm,
    it_hbm,
    ec_hbm,
    ic_hbm,
    send_hbm,
    out_ref,
    v0,
    src,
    tiles,
    cols,
    send_v,
    square,
    pick,
    w_hi,
    w_lo,
    pay,
    halo,
    vcat,
    hcat,
    vpart,
    part,
    psrc,
    load_sem,
    send_sem,
    recv_sem,
):
    partners, per_list = send_v.shape
    own = v0.shape[0]
    listed = partners * per_list
    blocks, slots, size, _ = et_hbm.shape
    ext_blocks = (own + listed) // size
    halves = v0.shape[1] // LANES
    exchanges = 2 * STEPS
    packed = listed // 2
    run = per_list // 2

    me = lax.axis_index("rows")
    targets = [lax.rem(me + partner_offset(o) + devices, devices) for o in range(partners)]

    barrier = pltpu.get_barrier_semaphore()
    for target in targets:
        pl.semaphore_signal(barrier, inc=1, device_id=(target,), device_id_type=MESH)

    loads = [
        pltpu.make_async_copy(send_hbm, send_v, load_sem.at[0]),
        pltpu.make_async_copy(v0_hbm, v0, load_sem.at[1]),
        pltpu.make_async_copy(et_hbm, tiles.at[0], load_sem.at[2]),
        pltpu.make_async_copy(ec_hbm, cols.at[0], load_sem.at[3]),
        pltpu.make_async_copy(src_hbm, src, load_sem.at[4]),
        pltpu.make_async_copy(it_hbm, tiles.at[1], load_sem.at[5]),
        pltpu.make_async_copy(ic_hbm, cols.at[1], load_sem.at[6]),
    ]
    for load in loads:
        load.start()

    def copies(exchange, group):
        return [
            pltpu.make_async_remote_copy(
                src_ref=pay.at[exchange, group, pl.ds(o * run, run)],
                dst_ref=halo.at[exchange, group, pl.ds(o * run, run)],
                send_sem=send_sem.at[exchange, group, o],
                recv_sem=recv_sem.at[exchange, group, o],
                device_id=(targets[o],),
                device_id_type=MESH,
            )
            for o in range(partners)
        ]

    def send(exchange, group):
        ready = copies(exchange, group)
        near = sorted(range(partners), key=lambda o: abs(partner_offset(o)))
        for core in range(2):
            order = sorted(near, key=lambda o: (partner_offset(o) + core) % 2)

            @pl.when(lax.rem(me, 2) == core)
            def _():
                for o in order:
                    ready[o].start()

    square[...] = jnp.zeros_like(square)
    loads[0].wait()
    square[0:partners, 0:per_list] = send_v[...].astype(F32)
    turned = square[...].T
    column = jnp.concatenate(
        [
            jnp.broadcast_to(turned[part_at * run : (part_at + 1) * run, o : o + 1], (run, LANES))
            for part_at in range(2)
            for o in range(partners)
        ],
        axis=0,
    )
    lane = lax.broadcasted_iota(jnp.int32, (listed, LANES), 1).astype(F32)
    for c in range(own // LANES):
        pick[:, c * LANES : (c + 1) * LANES] = jnp.where(
            column == lane + float(c * LANES), 1.0, 0.0
        ).astype(BF16)

    first = lax.broadcasted_iota(jnp.int32, (packed, LANES), 1) < LANES // 2

    def turn(x):
        return pltpu.roll(x, LANES // 2, 1)

    def pack(rows):
        one, two = rows[0:packed], rows[packed:]
        return jnp.where(first, one, turn(two)), jnp.where(first, turn(one), two)

    def unpack(x):
        turned_x = turn(x)
        lists = (partners, run, LANES)
        left = [jnp.where(first, y, 0.0).reshape(lists) for y in (x, turned_x)]
        right = [jnp.where(first, 0.0, y).reshape(lists) for y in (turned_x, x)]
        return [jnp.concatenate(y, axis=1).reshape(listed, LANES) for y in (left, right)]

    def picked(x):
        hi, mid = split2(x)
        low = ((x - hi.astype(F32)) - mid.astype(F32)).astype(BF16)
        wide = dot(pick[...], jnp.concatenate([hi, mid], axis=1))
        return (wide[:, :LANES] + wide[:, LANES:]) + dot(pick[...], low)

    loads[1].wait()
    for half in range(halves):
        groups = pack(picked(v0[:, half * LANES : (half + 1) * LANES]))
        for q in range(2):
            pay[0, 2 * half + q] = groups[q]
            if half == 0 and q == 0:
                pl.semaphore_wait(barrier, partners)
            send(0, 2 * half + q)

    def build(which):
        for g in range(blocks):
            named = [cols[which, g, k] for k in range(slots)]
            for c in range(ext_blocks):
                total = None
                for k in range(slots):
                    term = tiles[which, g, k] * jnp.where(named[k] == c, 1.0, 0.0).astype(F32)
                    total = term if total is None else total + term
                hi, lo = split2(total)
                rows = slice(listed + g * size, listed + (g + 1) * size)
                w_hi[which, rows, c * size : (c + 1) * size] = hi
                w_lo[which, rows, c * size : (c + 1) * size] = lo
        for w in (w_hi, w_lo):
            w[which, 0:listed] = dot(pick[...], w[which, listed:]).astype(BF16)

    loads[2].wait()
    loads[3].wait()
    build(0)
    loads[4].wait()
    for half in range(halves):
        psrc[half] = picked(src[:, half * LANES : (half + 1) * LANES])

    def own_part(which, half, state, exchange, with_source):
        hi, lo = split2(state)
        vcat[half, :, 0:LANES] = hi
        vcat[half, :, LANES:] = lo
        near = product(w_hi[which, :, 0:own], w_lo[which, :, 0:own], vcat[half])
        head, body = near[0:listed], state + near[listed:]
        if with_source:
            head = head + psrc[half]
            body = body + src[:, half * LANES : (half + 1) * LANES]
        groups = pack(head)
        for q in range(2):
            part[2 * half + q] = pay[exchange, 2 * half + q] + groups[q]
        vpart[half] = body

    for half in range(halves):
        own_part(0, half, v0[:, half * LANES : (half + 1) * LANES], 0, True)
    loads[5].wait()
    loads[6].wait()
    build(1)

    def stage(exchange, which, half, last):
        for q in range(2):
            group = 2 * half + q
            for copy in copies(exchange, group):
                copy.wait_recv()
            left, right = [
                jnp.concatenate(split2(x), axis=1) for x in unpack(halo[exchange, group])
            ]
            if not last:
                payload = part[group]
                wide = dot(w_hi[which, 0:packed, own:], left)
                wide = wide + dot(w_hi[which, packed:listed, own:], right)
                low = dot(w_lo[which, 0:packed, own:], left[:, :LANES])
                low = low + dot(w_lo[which, packed:listed, own:], right[:, :LANES])
                pay[exchange + 1, group] = payload + (
                    (wide[:, :LANES] + wide[:, LANES:]) + low
                )
                send(exchange + 1, group)
            if q == 0:
                hcat[...] = left
            else:
                hcat[...] = hcat[...] + right
        state = vpart[half] + product(
            w_hi[which, listed:, own:], w_lo[which, listed:, own:], hcat[...]
        )
        if last:
            out_ref[:, half * LANES : (half + 1) * LANES] = state
        else:
            own_part(1 - which, half, state, exchange + 1, which == 1)

    for exchange in range(exchanges):
        for half in range(halves):
            stage(exchange, exchange % 2, half, exchange == exchanges - 1)

    for exchange in range(exchanges):
        for group in range(2 * halves):
            for copy in copies(exchange, group):
                copy.wait_send()


def on_device(devices, v0, source, et, it, ec, ic, send):
    own, panels = v0.shape
    partners, per_list = send.shape
    blocks, slots, size, _ = et.shape
    listed = partners * per_list
    extended = own + listed
    halves = panels // LANES
    exchanges = 2 * STEPS
    in_hbm = pl.BlockSpec(memory_space=pltpu.HBM)
    return pl.pallas_call(
        functools.partial(kernel, devices),
        out_shape=jax.ShapeDtypeStruct((own, panels), F32),
        in_specs=[in_hbm] * 7,
        out_specs=pl.BlockSpec(memory_space=pltpu.VMEM),
        scratch_shapes=[
            pltpu.VMEM((own, panels), F32),
            pltpu.VMEM((own, panels), F32),
            pltpu.VMEM((2, blocks, slots, size, size), F32),
            pltpu.SMEM((2, blocks, slots), jnp.int32),
            pltpu.VMEM((partners, per_list), jnp.int32),
            pltpu.VMEM((LANES, LANES), F32),
            pltpu.VMEM((listed, own), BF16),
            pltpu.VMEM((2, extended, extended), BF16),
            pltpu.VMEM((2, extended, extended), BF16),
            pltpu.VMEM((exchanges, 2 * halves, listed // 2, LANES), F32),
            pltpu.VMEM((exchanges, 2 * halves, listed // 2, LANES), F32),
            pltpu.VMEM((halves, own, 2 * LANES), BF16),
            pltpu.VMEM((listed, 2 * LANES), BF16),
            pltpu.VMEM((halves, own, LANES), F32),
            pltpu.VMEM((2 * halves, listed // 2, LANES), F32),
            pltpu.VMEM((halves, listed, LANES), F32),
            pltpu.SemaphoreType.DMA((7,)),
            pltpu.SemaphoreType.DMA((exchanges, 2 * halves, partners)),
            pltpu.SemaphoreType.DMA((exchanges, 2 * halves, partners)),
        ],
        compiler_params=pltpu.CompilerParams(
            collective_id=0, has_side_effects=True, vmem_limit_bytes=48 * 1024 * 1024
        ),
    )(
        *[
            pltpu.with_memory_space_constraint(x, pltpu.HBM)
            for x in (v0, source, et, it, ec, ic, send)
        ]
    )


def solution(mesh):
    return jax.shard_map(
        functools.partial(on_device, mesh.shape["rows"]),
        mesh=mesh,
        in_specs=(
            P("rows", None),
            P("rows", None),
            P("rows", None, None, None),
            P("rows", None, None, None),
            P("rows", None),
            P("rows", None),
            P("rows", None),
        ),
        out_specs=P("rows", None),
        check_vma=False,
    )
```

```python
import functools

import jax
import jax.numpy as jnp
from jax import lax
from jax.experimental import pallas as pl
from jax.experimental.pallas import tpu as pltpu
from jax.sharding import PartitionSpec as P

STEPS = 3
LANES = 128
MESH = pl.DeviceIdType.MESH
F32 = jnp.float32
BF16 = jnp.bfloat16


def partner_offset(offset_index):
    return (offset_index // 2 + 1) * (1 if offset_index % 2 == 0 else -1)


def split2(x):
    hi = x.astype(BF16)
    lo = (x - hi.astype(F32)).astype(BF16)
    return hi, lo


def dot(a, b):
    return jnp.dot(a, b, preferred_element_type=F32)


def product(w_hi, w_lo, cat):
    wide = dot(w_hi, cat)
    return (wide[:, :LANES] + wide[:, LANES:]) + dot(w_lo, cat[:, :LANES])


def kernel(
    devices,
    v0_hbm,
    src_hbm,
    et_hbm,
    it_hbm,
    ec_hbm,
    ic_hbm,
    send_hbm,
    out_ref,
    v0,
    src,
    tiles,
    cols,
    send_v,
    square,
    pick,
    w_hi,
    w_lo,
    pay,
    halo,
    vcat,
    hcat,
    vpart,
    part,
    psrc,
    load_sem,
    send_sem,
    recv_sem,
):
    partners, per_list = send_v.shape
    own = v0.shape[0]
    listed = partners * per_list
    blocks, slots, size, _ = et_hbm.shape
    ext_blocks = (own + listed) // size
    halves = v0.shape[1] // LANES
    exchanges = 2 * STEPS
    packed = listed // 2
    run = per_list // 2

    me = lax.axis_index("rows")
    targets = [lax.rem(me + partner_offset(o) + devices, devices) for o in range(partners)]

    barrier = pltpu.get_barrier_semaphore()
    for target in targets:
        pl.semaphore_signal(barrier, inc=1, device_id=(target,), device_id_type=MESH)

    loads = [
        pltpu.make_async_copy(send_hbm, send_v, load_sem.at[0]),
        pltpu.make_async_copy(v0_hbm, v0, load_sem.at[1]),
        pltpu.make_async_copy(et_hbm, tiles.at[0], load_sem.at[2]),
        pltpu.make_async_copy(ec_hbm, cols.at[0], load_sem.at[3]),
        pltpu.make_async_copy(src_hbm, src, load_sem.at[4]),
        pltpu.make_async_copy(it_hbm, tiles.at[1], load_sem.at[5]),
        pltpu.make_async_copy(ic_hbm, cols.at[1], load_sem.at[6]),
    ]
    for load in loads:
        load.start()

    def copies(exchange, group):
        return [
            pltpu.make_async_remote_copy(
                src_ref=pay.at[exchange, group, pl.ds(o * run, run)],
                dst_ref=halo.at[exchange, group, pl.ds(o * run, run)],
                send_sem=send_sem.at[exchange],
                recv_sem=recv_sem.at[exchange % 2, group],
                device_id=(targets[o],),
                device_id_type=MESH,
            )
            for o in range(partners)
        ]

    def send(exchange, group):
        ready = copies(exchange, group)
        near = sorted(range(partners), key=lambda o: abs(partner_offset(o)))
        for core in range(2):
            order = sorted(near, key=lambda o: (partner_offset(o) + core) % 2)

            @pl.when(lax.rem(me, 2) == core)
            def _():
                for o in order:
                    ready[o].start()

    square[...] = jnp.zeros_like(square)
    loads[0].wait()
    square[0:partners, 0:per_list] = send_v[...].astype(F32)
    turned = square[...].T
    column = jnp.concatenate(
        [
            jnp.broadcast_to(turned[part_at * run : (part_at + 1) * run, o : o + 1], (run, LANES))
            for part_at in range(2)
            for o in range(partners)
        ],
        axis=0,
    )
    lane = lax.broadcasted_iota(jnp.int32, (listed, LANES), 1).astype(F32)
    for c in range(own // LANES):
        pick[:, c * LANES : (c + 1) * LANES] = jnp.where(
            column == lane + float(c * LANES), 1.0, 0.0
        ).astype(BF16)

    first = lax.broadcasted_iota(jnp.int32, (packed, LANES), 1) < LANES // 2

    def turn(x):
        return pltpu.roll(x, LANES // 2, 1)

    def pack(rows):
        one, two = rows[0:packed], rows[packed:]
        return jnp.where(first, one, turn(two)), jnp.where(first, turn(one), two)

    def unpack(x):
        turned_x = turn(x)
        lists = (partners, run, LANES)
        left = [jnp.where(first, y, 0.0).reshape(lists) for y in (x, turned_x)]
        right = [jnp.where(first, 0.0, y).reshape(lists) for y in (turned_x, x)]
        return [jnp.concatenate(y, axis=1).reshape(listed, LANES) for y in (left, right)]

    def picked(x):
        hi, mid = split2(x)
        low = ((x - hi.astype(F32)) - mid.astype(F32)).astype(BF16)
        wide = dot(pick[...], jnp.concatenate([hi, mid], axis=1))
        return (wide[:, :LANES] + wide[:, LANES:]) + dot(pick[...], low)

    loads[1].wait()
    for half in range(halves):
        groups = pack(picked(v0[:, half * LANES : (half + 1) * LANES]))
        for q in range(2):
            pay[0, 2 * half + q] = groups[q]
            if half == 0 and q == 0:
                pl.semaphore_wait(barrier, partners)
            send(0, 2 * half + q)

    def build(which):
        for g in range(blocks):
            named = [cols[which, g, k] for k in range(slots)]
            for c in range(ext_blocks):
                total = None
                for k in range(slots):
                    term = tiles[which, g, k] * jnp.where(named[k] == c, 1.0, 0.0).astype(F32)
                    total = term if total is None else total + term
                hi, lo = split2(total)
                rows = slice(listed + g * size, listed + (g + 1) * size)
                w_hi[which, rows, c * size : (c + 1) * size] = hi
                w_lo[which, rows, c * size : (c + 1) * size] = lo
        for w in (w_hi, w_lo):
            w[which, 0:listed] = dot(pick[...], w[which, listed:]).astype(BF16)

    loads[2].wait()
    loads[3].wait()
    build(0)
    loads[4].wait()
    for half in range(halves):
        psrc[half] = picked(src[:, half * LANES : (half + 1) * LANES])

    def own_part(which, half, state, exchange, with_source):
        hi, lo = split2(state)
        vcat[half, :, 0:LANES] = hi
        vcat[half, :, LANES:] = lo
        near = product(w_hi[which, :, 0:own], w_lo[which, :, 0:own], vcat[half])
        head, body = near[0:listed], state + near[listed:]
        if with_source:
            head = head + psrc[half]
            body = body + src[:, half * LANES : (half + 1) * LANES]
        groups = pack(head)
        for q in range(2):
            part[2 * half + q] = pay[exchange, 2 * half + q] + groups[q]
        vpart[half] = body

    for half in range(halves):
        own_part(0, half, v0[:, half * LANES : (half + 1) * LANES], 0, True)
    loads[5].wait()
    loads[6].wait()
    build(1)

    def stage(exchange, which, half, last):
        for q in range(2):
            group = 2 * half + q
            arrived = halo.at[exchange, group]
            pltpu.make_async_copy(arrived, arrived, recv_sem.at[exchange % 2, group]).wait()
            left, right = [
                jnp.concatenate(split2(x), axis=1) for x in unpack(halo[exchange, group])
            ]
            if not last:
                payload = part[group]
                wide = dot(w_hi[which, 0:packed, own:], left)
                wide = wide + dot(w_hi[which, packed:listed, own:], right)
                low = dot(w_lo[which, 0:packed, own:], left[:, :LANES])
                low = low + dot(w_lo[which, packed:listed, own:], right[:, :LANES])
                pay[exchange + 1, group] = payload + (
                    (wide[:, :LANES] + wide[:, LANES:]) + low
                )
                send(exchange + 1, group)
            if q == 0:
                hcat[...] = left
            else:
                hcat[...] = hcat[...] + right
        state = vpart[half] + product(
            w_hi[which, listed:, own:], w_lo[which, listed:, own:], hcat[...]
        )
        if last:
            out_ref[:, half * LANES : (half + 1) * LANES] = state
        else:
            own_part(1 - which, half, state, exchange + 1, which == 1)

    for exchange in range(exchanges):
        for half in range(halves):
            stage(exchange, exchange % 2, half, exchange == exchanges - 1)

    for exchange in range(exchanges):
        sent = pay.at[exchange]
        pltpu.make_async_copy(sent, sent, send_sem.at[exchange]).wait()


def on_device(devices, v0, source, et, it, ec, ic, send):
    own, panels = v0.shape
    partners, per_list = send.shape
    blocks, slots, size, _ = et.shape
    listed = partners * per_list
    extended = own + listed
    halves = panels // LANES
    exchanges = 2 * STEPS
    in_hbm = pl.BlockSpec(memory_space=pltpu.HBM)
    return pl.pallas_call(
        functools.partial(kernel, devices),
        out_shape=jax.ShapeDtypeStruct((own, panels), F32),
        in_specs=[in_hbm] * 7,
        out_specs=pl.BlockSpec(memory_space=pltpu.VMEM),
        scratch_shapes=[
            pltpu.VMEM((own, panels), F32),
            pltpu.VMEM((own, panels), F32),
            pltpu.VMEM((2, blocks, slots, size, size), F32),
            pltpu.SMEM((2, blocks, slots), jnp.int32),
            pltpu.VMEM((partners, per_list), jnp.int32),
            pltpu.VMEM((LANES, LANES), F32),
            pltpu.VMEM((listed, own), BF16),
            pltpu.VMEM((2, extended, extended), BF16),
            pltpu.VMEM((2, extended, extended), BF16),
            pltpu.VMEM((exchanges, 2 * halves, listed // 2, LANES), F32),
            pltpu.VMEM((exchanges, 2 * halves, listed // 2, LANES), F32),
            pltpu.VMEM((halves, own, 2 * LANES), BF16),
            pltpu.VMEM((listed, 2 * LANES), BF16),
            pltpu.VMEM((halves, own, LANES), F32),
            pltpu.VMEM((2 * halves, listed // 2, LANES), F32),
            pltpu.VMEM((halves, listed, LANES), F32),
            pltpu.SemaphoreType.DMA((7,)),
            pltpu.SemaphoreType.DMA((exchanges,)),
            pltpu.SemaphoreType.DMA((2, 2 * halves)),
        ],
        compiler_params=pltpu.CompilerParams(
            collective_id=0, has_side_effects=True, vmem_limit_bytes=48 * 1024 * 1024
        ),
    )(
        *[
            pltpu.with_memory_space_constraint(x, pltpu.HBM)
            for x in (v0, source, et, it, ec, ic, send)
        ]
    )


def solution(mesh):
    return jax.shard_map(
        functools.partial(on_device, mesh.shape["rows"]),
        mesh=mesh,
        in_specs=(
            P("rows", None),
            P("rows", None),
            P("rows", None, None, None),
            P("rows", None, None, None),
            P("rows", None),
            P("rows", None),
            P("rows", None),
        ),
        out_specs=P("rows", None),
        check_vma=False,
    )
```

```python
import functools

import jax
import jax.numpy as jnp
from jax import lax
from jax.experimental import pallas as pl
from jax.experimental.pallas import tpu as pltpu
from jax.sharding import PartitionSpec as P

STEPS = 3
LANES = 128
MESH = pl.DeviceIdType.MESH
F32 = jnp.float32
BF16 = jnp.bfloat16


def partner_offset(offset_index):
    return (offset_index // 2 + 1) * (1 if offset_index % 2 == 0 else -1)


def split2(x):
    hi = x.astype(BF16)
    lo = (x - hi.astype(F32)).astype(BF16)
    return hi, lo


def dot(a, b):
    return jnp.dot(a, b, preferred_element_type=F32)


def product(w_hi, w_lo, cat):
    wide = dot(w_hi, cat)
    return (wide[:, :LANES] + wide[:, LANES:]) + dot(w_lo, cat[:, :LANES])


def kernel(
    devices,
    v0_hbm,
    src_hbm,
    et_hbm,
    it_hbm,
    ec_hbm,
    ic_hbm,
    send_hbm,
    out_ref,
    v0,
    src,
    tiles,
    cols,
    send_v,
    square,
    pick,
    w_hi,
    w_lo,
    u_hi,
    u_lo,
    pay,
    halo,
    vcat,
    hcat,
    vpart,
    part,
    psrc,
    load_sem,
    send_sem,
    recv_sem,
):
    partners, per_list = send_v.shape
    own = v0.shape[0]
    listed = partners * per_list
    blocks, slots, size, _ = et_hbm.shape
    ext_blocks = (own + listed) // size
    halves = v0.shape[1] // LANES
    exchanges = 2 * STEPS
    packed = listed // 2
    run = per_list // 2

    me = lax.axis_index("rows")
    targets = [lax.rem(me + partner_offset(o) + devices, devices) for o in range(partners)]

    barrier = pltpu.get_barrier_semaphore()
    for target in targets:
        pl.semaphore_signal(barrier, inc=1, device_id=(target,), device_id_type=MESH)

    loads = [
        pltpu.make_async_copy(send_hbm, send_v, load_sem.at[0]),
        pltpu.make_async_copy(v0_hbm, v0, load_sem.at[1]),
        pltpu.make_async_copy(et_hbm, tiles.at[0], load_sem.at[2]),
        pltpu.make_async_copy(ec_hbm, cols.at[0], load_sem.at[3]),
        pltpu.make_async_copy(src_hbm, src, load_sem.at[4]),
        pltpu.make_async_copy(it_hbm, tiles.at[1], load_sem.at[5]),
        pltpu.make_async_copy(ic_hbm, cols.at[1], load_sem.at[6]),
    ]
    for load in loads:
        load.start()

    def copies(exchange, group):
        return [
            pltpu.make_async_remote_copy(
                src_ref=pay.at[exchange, group, pl.ds(o * run, run)],
                dst_ref=halo.at[exchange, group, pl.ds(o * run, run)],
                send_sem=send_sem.at[exchange],
                recv_sem=recv_sem.at[exchange % 2, group],
                device_id=(targets[o],),
                device_id_type=MESH,
            )
            for o in range(partners)
        ]

    def send(exchange, group):
        ready = copies(exchange, group)
        near = sorted(range(partners), key=lambda o: abs(partner_offset(o)))
        for core in range(2):
            order = sorted(near, key=lambda o: (partner_offset(o) + core) % 2)

            @pl.when(lax.rem(me, 2) == core)
            def _():
                for o in order:
                    ready[o].start()

    square[...] = jnp.zeros_like(square)
    loads[0].wait()
    square[0:partners, 0:per_list] = send_v[...].astype(F32)
    turned = square[...].T
    column = jnp.concatenate(
        [
            jnp.broadcast_to(turned[part_at * run : (part_at + 1) * run, o : o + 1], (run, LANES))
            for part_at in range(2)
            for o in range(partners)
        ],
        axis=0,
    )
    lane = lax.broadcasted_iota(jnp.int32, (listed, LANES), 1).astype(F32)
    for c in range(own // LANES):
        pick[:, c * LANES : (c + 1) * LANES] = jnp.where(
            column == lane + float(c * LANES), 1.0, 0.0
        ).astype(BF16)

    first = lax.broadcasted_iota(jnp.int32, (packed, LANES), 1) < LANES // 2

    def turn(x):
        return pltpu.roll(x, LANES // 2, 1)

    def pack(rows):
        one, two = rows[0:packed], rows[packed:]
        return jnp.where(first, one, turn(two)), jnp.where(first, turn(one), two)

    def unpack(x):
        turned_x = turn(x)
        lists = (partners, run, LANES)
        left = [jnp.where(first, y, 0.0).reshape(lists) for y in (x, turned_x)]
        right = [jnp.where(first, 0.0, y).reshape(lists) for y in (turned_x, x)]
        return [jnp.concatenate(y, axis=1).reshape(listed, LANES) for y in (left, right)]

    def picked(x):
        hi, mid = split2(x)
        low = ((x - hi.astype(F32)) - mid.astype(F32)).astype(BF16)
        wide = dot(pick[...], jnp.concatenate([hi, mid], axis=1))
        return (wide[:, :LANES] + wide[:, LANES:]) + dot(pick[...], low)

    loads[1].wait()
    for half in range(halves):
        groups = pack(picked(v0[:, half * LANES : (half + 1) * LANES]))
        for q in range(2):
            pay[0, 2 * half + q] = groups[q]
            if half == 0 and q == 0:
                pl.semaphore_wait(barrier, partners)
            send(0, 2 * half + q)

    def build(which):
        for g in range(blocks):
            named = [cols[which, g, k] for k in range(slots)]
            for c in range(ext_blocks):
                total = None
                for k in range(slots):
                    term = tiles[which, g, k] * jnp.where(named[k] == c, 1.0, 0.0).astype(F32)
                    total = term if total is None else total + term
                hi, lo = split2(total)
                rows = slice(listed + g * size, listed + (g + 1) * size)
                w_hi[which, rows, c * size : (c + 1) * size] = hi
                w_lo[which, rows, c * size : (c + 1) * size] = lo
        for w, u in ((w_hi, u_hi), (w_lo, u_lo)):
            top = dot(pick[...], w[which, listed:]).astype(BF16)
            w[which, 0:listed, 0:own] = top[:, 0:own]
            u[which, :, 0:listed] = top[0:packed, own:]
            u[which, :, listed:] = top[packed:, own:]

    loads[2].wait()
    loads[3].wait()
    build(0)
    loads[4].wait()
    for half in range(halves):
        psrc[half] = picked(src[:, half * LANES : (half + 1) * LANES])

    def source_of(half):
        return src[:, half * LANES : (half + 1) * LANES]

    def settle(half, state, add_source):
        hi, lo = split2(state)
        vcat[half, :, 0:LANES] = hi
        vcat[half, :, LANES:] = lo
        vpart[half] = state + source_of(half) if add_source else state

    def near_head(which, half, exchange, add_source):
        head = product(w_hi[which, 0:listed, 0:own], w_lo[which, 0:listed, 0:own], vcat[half])
        groups = pack(head + psrc[half] if add_source else head)
        for q in range(2):
            part[2 * half + q] = pay[exchange, 2 * half + q] + groups[q]

    def near_body(which, half):
        vpart[half] = vpart[half] + product(
            w_hi[which, listed:, 0:own], w_lo[which, listed:, 0:own], vcat[half]
        )

    for half in range(halves):
        settle(half, v0[:, half * LANES : (half + 1) * LANES], True)
        near_head(0, half, 0, True)
        near_body(0, half)
    loads[5].wait()
    loads[6].wait()
    build(1)

    def urgent(exchange, which, group, last):
        arrived = halo.at[exchange, group]
        pltpu.make_async_copy(arrived, arrived, recv_sem.at[exchange % 2, group]).wait()
        left, right = [jnp.concatenate(split2(x), axis=1) for x in unpack(arrived[...])]
        if not last:
            both = jnp.concatenate([left, right], axis=0)
            wide = dot(u_hi[which], both)
            low = dot(u_lo[which], both[:, :LANES])
            pay[exchange + 1, group] = part[group] + ((wide[:, :LANES] + wide[:, LANES:]) + low)
            send(exchange + 1, group)
        if group % 2 == 0:
            hcat[...] = left
        else:
            hcat[...] = hcat[...] + right

    def far_body(which, half):
        return vpart[half] + product(
            w_hi[which, listed:, own:], w_lo[which, listed:, own:], hcat[...]
        )

    waiting = []
    for exchange in range(exchanges):
        which = exchange % 2
        last = exchange == exchanges - 1
        for group in range(2 * halves):
            urgent(exchange, which, group, last)
            if waiting:
                waiting.pop(0)()
            if group % 2 == 1:
                half = group // 2
                state = far_body(which, half)
                if last:
                    out_ref[:, half * LANES : (half + 1) * LANES] = state
                    continue
                settle(half, state, which == 1)
                waiting.append(
                    functools.partial(near_head, 1 - which, half, exchange + 1, which == 1)
                )
                waiting.append(functools.partial(near_body, 1 - which, half))

    for exchange in range(exchanges):
        sent = pay.at[exchange]
        pltpu.make_async_copy(sent, sent, send_sem.at[exchange]).wait()


def on_device(devices, v0, source, et, it, ec, ic, send):
    own, panels = v0.shape
    partners, per_list = send.shape
    blocks, slots, size, _ = et.shape
    listed = partners * per_list
    extended = own + listed
    halves = panels // LANES
    exchanges = 2 * STEPS
    in_hbm = pl.BlockSpec(memory_space=pltpu.HBM)
    return pl.pallas_call(
        functools.partial(kernel, devices),
        out_shape=jax.ShapeDtypeStruct((own, panels), F32),
        in_specs=[in_hbm] * 7,
        out_specs=pl.BlockSpec(memory_space=pltpu.VMEM),
        scratch_shapes=[
            pltpu.VMEM((own, panels), F32),
            pltpu.VMEM((own, panels), F32),
            pltpu.VMEM((2, blocks, slots, size, size), F32),
            pltpu.SMEM((2, blocks, slots), jnp.int32),
            pltpu.VMEM((partners, per_list), jnp.int32),
            pltpu.VMEM((LANES, LANES), F32),
            pltpu.VMEM((listed, own), BF16),
            pltpu.VMEM((2, extended, extended), BF16),
            pltpu.VMEM((2, extended, extended), BF16),
            pltpu.VMEM((2, listed // 2, 2 * listed), BF16),
            pltpu.VMEM((2, listed // 2, 2 * listed), BF16),
            pltpu.VMEM((exchanges, 2 * halves, listed // 2, LANES), F32),
            pltpu.VMEM((exchanges, 2 * halves, listed // 2, LANES), F32),
            pltpu.VMEM((halves, own, 2 * LANES), BF16),
            pltpu.VMEM((listed, 2 * LANES), BF16),
            pltpu.VMEM((halves, own, LANES), F32),
            pltpu.VMEM((2 * halves, listed // 2, LANES), F32),
            pltpu.VMEM((halves, listed, LANES), F32),
            pltpu.SemaphoreType.DMA((7,)),
            pltpu.SemaphoreType.DMA((exchanges,)),
            pltpu.SemaphoreType.DMA((2, 2 * halves)),
        ],
        compiler_params=pltpu.CompilerParams(
            collective_id=0, has_side_effects=True, vmem_limit_bytes=48 * 1024 * 1024
        ),
    )(
        *[
            pltpu.with_memory_space_constraint(x, pltpu.HBM)
            for x in (v0, source, et, it, ec, ic, send)
        ]
    )


def solution(mesh):
    return jax.shard_map(
        functools.partial(on_device, mesh.shape["rows"]),
        mesh=mesh,
        in_specs=(
            P("rows", None),
            P("rows", None),
            P("rows", None, None, None),
            P("rows", None, None, None),
            P("rows", None),
            P("rows", None),
            P("rows", None),
        ),
        out_specs=P("rows", None),
        check_vma=False,
    )
```

```python
import functools

import jax
import jax.numpy as jnp
from jax import lax
from jax.experimental import pallas as pl
from jax.experimental.pallas import tpu as pltpu
from jax.sharding import PartitionSpec as P

STEPS = 3
LANES = 128
MESH = pl.DeviceIdType.MESH
F32 = jnp.float32
BF16 = jnp.bfloat16


def split2(x):
    hi = x.astype(BF16)
    lo = (x - hi.astype(F32)).astype(BF16)
    return hi, lo


def dot(a, b):
    return jnp.dot(a, b, preferred_element_type=F32)


def product(w_hi, w_lo, cat):
    wide = dot(w_hi, cat)
    return (wide[:, :LANES] + wide[:, LANES:]) + dot(w_lo, cat[:, :LANES])


def kernel(
    devices,
    v0_hbm,
    src_hbm,
    et_hbm,
    it_hbm,
    ec_hbm,
    ic_hbm,
    send_hbm,
    out_ref,
    v0,
    src,
    tiles,
    cols,
    send_v,
    square,
    pick,
    w_hi,
    w_lo,
    u_hi,
    u_lo,
    pay,
    halo,
    vcat,
    hcat,
    vpart,
    part,
    psrc,
    load_sem,
    send_sem,
    recv_sem,
):
    partners, per_list = send_v.shape
    own = v0.shape[0]
    listed = partners * per_list
    blocks, slots, size, _ = et_hbm.shape
    ext_blocks = (own + listed) // size
    halves = v0.shape[1] // LANES
    exchanges = 2 * STEPS
    packed = listed // 2
    run = per_list // 2

    me = lax.axis_index("rows")
    core = lax.rem(me, 2)
    reach = [4 * (p // 2 % (partners // 4)) // 2 + 1 for p in range(partners)]
    late = [core if p < partners // 2 else 1 - core for p in range(partners)]
    reach = [reach[p] + 1 - late[p] for p in range(partners)]
    list_at = [2 * (reach[p] - 1) + p % 2 for p in range(partners)]
    targets = [
        lax.rem(me + (reach[p] if p % 2 == 0 else devices - reach[p]), devices)
        for p in range(partners)
    ]

    barrier = pltpu.get_barrier_semaphore()
    for target in targets:
        pl.semaphore_signal(barrier, inc=1, device_id=(target,), device_id_type=MESH)

    loads = [
        pltpu.make_async_copy(send_hbm, send_v, load_sem.at[0]),
        pltpu.make_async_copy(v0_hbm, v0, load_sem.at[1]),
        pltpu.make_async_copy(et_hbm, tiles.at[0], load_sem.at[2]),
        pltpu.make_async_copy(ec_hbm, cols.at[0], load_sem.at[3]),
        pltpu.make_async_copy(src_hbm, src, load_sem.at[4]),
        pltpu.make_async_copy(it_hbm, tiles.at[1], load_sem.at[5]),
        pltpu.make_async_copy(ic_hbm, cols.at[1], load_sem.at[6]),
    ]
    for load in loads:
        load.start()

    def send(exchange, group, first, last):
        for p in range(first, last):
            pltpu.make_async_remote_copy(
                src_ref=pay.at[exchange, group, pl.ds(p * run, run)],
                dst_ref=halo.at[exchange, group, pl.ds(pl.multiple_of(list_at[p] * run, 8), run)],
                send_sem=send_sem.at[exchange],
                recv_sem=recv_sem.at[exchange % 2, group],
                device_id=(targets[p],),
                device_id_type=MESH,
            ).start()

    square[...] = jnp.zeros_like(square)
    loads[0].wait()
    for p in range(partners):
        square[p : p + 1, 0:per_list] = send_v[pl.ds(list_at[p], 1), :].astype(F32)
    turned = square[...].T
    column = jnp.concatenate(
        [
            jnp.broadcast_to(turned[part_at * run : (part_at + 1) * run, p : p + 1], (run, LANES))
            for part_at in range(2)
            for p in range(partners)
        ],
        axis=0,
    )
    lane = lax.broadcasted_iota(jnp.int32, (listed, LANES), 1).astype(F32)
    for c in range(own // LANES):
        pick[:, c * LANES : (c + 1) * LANES] = jnp.where(
            column == lane + float(c * LANES), 1.0, 0.0
        ).astype(BF16)

    first = lax.broadcasted_iota(jnp.int32, (packed, LANES), 1) < LANES // 2

    def turn(x):
        return pltpu.roll(x, LANES // 2, 1)

    def pack(rows):
        one, two = rows[0:packed], rows[packed:]
        return jnp.where(first, one, turn(two)), jnp.where(first, turn(one), two)

    def unpack(x):
        turned_x = turn(x)
        lists = (partners, run, LANES)
        left = [jnp.where(first, y, 0.0).reshape(lists) for y in (x, turned_x)]
        right = [jnp.where(first, 0.0, y).reshape(lists) for y in (turned_x, x)]
        return [jnp.concatenate(y, axis=1).reshape(listed, LANES) for y in (left, right)]

    def picked(x):
        hi, mid = split2(x)
        low = ((x - hi.astype(F32)) - mid.astype(F32)).astype(BF16)
        wide = dot(pick[...], jnp.concatenate([hi, mid], axis=1))
        return (wide[:, :LANES] + wide[:, LANES:]) + dot(pick[...], low)

    loads[1].wait()
    for half in range(halves):
        groups = pack(picked(v0[:, half * LANES : (half + 1) * LANES]))
        for q in range(2):
            pay[0, 2 * half + q] = groups[q]
            if half == 0 and q == 0:
                pl.semaphore_wait(barrier, partners)
            send(0, 2 * half + q, 0, partners)

    def build(which):
        for g in range(blocks):
            named = [cols[which, g, k] for k in range(slots)]
            for c in range(ext_blocks):
                total = None
                for k in range(slots):
                    term = tiles[which, g, k] * jnp.where(named[k] == c, 1.0, 0.0).astype(F32)
                    total = term if total is None else total + term
                hi, lo = split2(total)
                rows = slice(listed + g * size, listed + (g + 1) * size)
                w_hi[which, rows, c * size : (c + 1) * size] = hi
                w_lo[which, rows, c * size : (c + 1) * size] = lo
        for w, u in ((w_hi, u_hi), (w_lo, u_lo)):
            top = dot(pick[...], w[which, listed:]).astype(BF16)
            w[which, 0:listed, 0:own] = top[:, 0:own]
            u[which, :, 0:listed] = top[0:packed, own:]
            u[which, :, listed:] = top[packed:, own:]

    loads[2].wait()
    loads[3].wait()
    build(0)
    loads[4].wait()
    for half in range(halves):
        psrc[half] = picked(src[:, half * LANES : (half + 1) * LANES])

    def source_of(half):
        return src[:, half * LANES : (half + 1) * LANES]

    def settle(half, state, add_source):
        hi, lo = split2(state)
        vcat[half, :, 0:LANES] = hi
        vcat[half, :, LANES:] = lo
        vpart[half] = state + source_of(half) if add_source else state

    def near_head(which, half, exchange, add_source):
        head = product(w_hi[which, 0:listed, 0:own], w_lo[which, 0:listed, 0:own], vcat[half])
        groups = pack(head + psrc[half] if add_source else head)
        for q in range(2):
            part[2 * half + q] = pay[exchange, 2 * half + q] + groups[q]

    def near_body(which, half):
        vpart[half] = vpart[half] + product(
            w_hi[which, listed:, 0:own], w_lo[which, listed:, 0:own], vcat[half]
        )

    for half in range(halves):
        settle(half, v0[:, half * LANES : (half + 1) * LANES], True)
        near_head(0, half, 0, True)
        near_body(0, half)
    loads[5].wait()
    loads[6].wait()
    build(1)

    def urgent(exchange, which, group, last):
        arrived = halo.at[exchange, group]
        pltpu.make_async_copy(arrived, arrived, recv_sem.at[exchange % 2, group]).wait()
        left, right = [jnp.concatenate(split2(x), axis=1) for x in unpack(arrived[...])]
        if not last:
            both = jnp.concatenate([left, right], axis=0)
            for chunk in range(2):
                rows = slice(chunk * packed // 2, (chunk + 1) * packed // 2)
                pay[exchange + 1, group, rows] = part[group, rows] + product(
                    u_hi[which, rows], u_lo[which, rows], both
                )
                send(
                    exchange + 1, group, chunk * partners // 2, (chunk + 1) * partners // 2
                )
        if group % 2 == 0:
            hcat[...] = left
        else:
            hcat[...] = hcat[...] + right

    def far_body(which, half):
        return vpart[half] + product(
            w_hi[which, listed:, own:], w_lo[which, listed:, own:], hcat[...]
        )

    waiting = []
    for exchange in range(exchanges):
        which = exchange % 2
        last = exchange == exchanges - 1
        for group in range(2 * halves):
            urgent(exchange, which, group, last)
            if waiting:
                waiting.pop(0)()
            if group % 2 == 1:
                half = group // 2
                state = far_body(which, half)
                if last:
                    out_ref[:, half * LANES : (half + 1) * LANES] = state
                    continue
                settle(half, state, which == 1)
                if exchange + 2 < exchanges:
                    waiting.append(
                        functools.partial(near_head, 1 - which, half, exchange + 1, which == 1)
                    )
                waiting.append(functools.partial(near_body, 1 - which, half))

    for exchange in range(exchanges):
        sent = pay.at[exchange]
        pltpu.make_async_copy(sent, sent, send_sem.at[exchange]).wait()


def on_device(devices, v0, source, et, it, ec, ic, send):
    own, panels = v0.shape
    partners, per_list = send.shape
    blocks, slots, size, _ = et.shape
    listed = partners * per_list
    extended = own + listed
    halves = panels // LANES
    exchanges = 2 * STEPS
    in_hbm = pl.BlockSpec(memory_space=pltpu.HBM)
    return pl.pallas_call(
        functools.partial(kernel, devices),
        out_shape=jax.ShapeDtypeStruct((own, panels), F32),
        in_specs=[in_hbm] * 7,
        out_specs=pl.BlockSpec(memory_space=pltpu.VMEM),
        scratch_shapes=[
            pltpu.VMEM((own, panels), F32),
            pltpu.VMEM((own, panels), F32),
            pltpu.VMEM((2, blocks, slots, size, size), F32),
            pltpu.SMEM((2, blocks, slots), jnp.int32),
            pltpu.VMEM((partners, per_list), jnp.int32),
            pltpu.VMEM((LANES, LANES), F32),
            pltpu.VMEM((listed, own), BF16),
            pltpu.VMEM((2, extended, extended), BF16),
            pltpu.VMEM((2, extended, extended), BF16),
            pltpu.VMEM((2, listed // 2, 2 * listed), BF16),
            pltpu.VMEM((2, listed // 2, 2 * listed), BF16),
            pltpu.VMEM((exchanges, 2 * halves, listed // 2, LANES), F32),
            pltpu.VMEM((exchanges, 2 * halves, listed // 2, LANES), F32),
            pltpu.VMEM((halves, own, 2 * LANES), BF16),
            pltpu.VMEM((listed, 2 * LANES), BF16),
            pltpu.VMEM((halves, own, LANES), F32),
            pltpu.VMEM((2 * halves, listed // 2, LANES), F32),
            pltpu.VMEM((halves, listed, LANES), F32),
            pltpu.SemaphoreType.DMA((7,)),
            pltpu.SemaphoreType.DMA((exchanges,)),
            pltpu.SemaphoreType.DMA((2, 2 * halves)),
        ],
        compiler_params=pltpu.CompilerParams(
            collective_id=0, has_side_effects=True, vmem_limit_bytes=48 * 1024 * 1024
        ),
    )(
        *[
            pltpu.with_memory_space_constraint(x, pltpu.HBM)
            for x in (v0, source, et, it, ec, ic, send)
        ]
    )


def solution(mesh):
    return jax.shard_map(
        functools.partial(on_device, mesh.shape["rows"]),
        mesh=mesh,
        in_specs=(
            P("rows", None),
            P("rows", None),
            P("rows", None, None, None),
            P("rows", None, None, None),
            P("rows", None),
            P("rows", None),
            P("rows", None),
        ),
        out_specs=P("rows", None),
        check_vma=False,
    )
```

```python
import functools

import jax
import jax.numpy as jnp
from jax import lax
from jax.experimental import pallas as pl
from jax.experimental.pallas import tpu as pltpu
from jax.sharding import PartitionSpec as P

STEPS = 3
LANES = 128
MESH = pl.DeviceIdType.MESH
F32 = jnp.float32
BF16 = jnp.bfloat16


def split2(x):
    hi = x.astype(BF16)
    lo = (x - hi.astype(F32)).astype(BF16)
    return hi, lo


def dot(a, b):
    return jnp.dot(a, b, preferred_element_type=F32)


def product(w_hi, w_lo, cat):
    wide = dot(w_hi, cat)
    return (wide[:, :LANES] + wide[:, LANES:]) + dot(w_lo, cat[:, :LANES])


def kernel(
    devices,
    v0_hbm,
    src_hbm,
    et_hbm,
    it_hbm,
    ec_hbm,
    ic_hbm,
    send_hbm,
    out_ref,
    v0,
    src,
    tiles,
    cols,
    send_v,
    square,
    pick,
    move,
    w_hi,
    w_lo,
    u_hi,
    u_lo,
    pay,
    halo,
    vcat,
    hcat,
    vpart,
    part,
    psrc,
    load_sem,
    send_sem,
    recv_sem,
):
    partners, per_list = send_v.shape
    own = v0.shape[0]
    listed = partners * per_list
    blocks, slots, size, _ = et_hbm.shape
    ext_blocks = (own + listed) // size
    halves = v0.shape[1] // LANES
    exchanges = 2 * STEPS
    packed = listed // 2
    run = per_list // 2

    me = lax.axis_index("rows")
    core = lax.rem(me, 2)
    reach = [4 * (p // 2 % (partners // 4)) // 2 + 1 for p in range(partners)]
    late = [core if p < partners // 2 else 1 - core for p in range(partners)]
    reach = [reach[p] + 1 - late[p] for p in range(partners)]
    list_at = [2 * (reach[p] - 1) + p % 2 for p in range(partners)]
    targets = [
        lax.rem(me + (reach[p] if p % 2 == 0 else devices - reach[p]), devices)
        for p in range(partners)
    ]

    barrier = pltpu.get_barrier_semaphore()
    for target in targets:
        pl.semaphore_signal(barrier, inc=1, device_id=(target,), device_id_type=MESH)

    loads = [
        pltpu.make_async_copy(send_hbm, send_v, load_sem.at[0]),
        pltpu.make_async_copy(v0_hbm, v0, load_sem.at[1]),
        pltpu.make_async_copy(et_hbm, tiles.at[0], load_sem.at[2]),
        pltpu.make_async_copy(ec_hbm, cols.at[0], load_sem.at[3]),
        pltpu.make_async_copy(src_hbm, src, load_sem.at[4]),
        pltpu.make_async_copy(it_hbm, tiles.at[1], load_sem.at[5]),
        pltpu.make_async_copy(ic_hbm, cols.at[1], load_sem.at[6]),
    ]
    for load in loads:
        load.start()

    def send(exchange, group):
        for p in range(partners):
            pltpu.make_async_remote_copy(
                src_ref=pay.at[exchange, group, pl.ds(p * run, run)],
                dst_ref=halo.at[exchange, group, pl.ds(pl.multiple_of(list_at[p] * run, 8), run)],
                send_sem=send_sem.at[exchange],
                recv_sem=recv_sem.at[exchange % 2, group],
                device_id=(targets[p],),
                device_id_type=MESH,
            ).start()

    square[...] = jnp.zeros_like(square)
    loads[0].wait()
    for p in range(partners):
        square[p : p + 1, 0:per_list] = send_v[pl.ds(list_at[p], 1), :].astype(F32)
    turned = square[...].T
    column = jnp.concatenate(
        [
            jnp.broadcast_to(turned[part_at * run : (part_at + 1) * run, p : p + 1], (run, LANES))
            for part_at in range(2)
            for p in range(partners)
        ],
        axis=0,
    )
    lane = lax.broadcasted_iota(jnp.int32, (listed, LANES), 1).astype(F32)
    for c in range(own // LANES):
        pick[:, c * LANES : (c + 1) * LANES] = jnp.where(
            column == lane + float(c * LANES), 1.0, 0.0
        ).astype(BF16)

    first = lax.broadcasted_iota(jnp.int32, (packed, LANES), 1) < LANES // 2

    def turn(x):
        return pltpu.roll(x, LANES // 2, 1)

    def pack(rows):
        one, two = rows[0:packed], rows[packed:]
        return jnp.where(first, one, turn(two)), jnp.where(first, turn(one), two)

    def unpack(x):
        turned_x = turn(x)
        direct = jnp.concatenate([jnp.where(first, x, 0.0), jnp.where(first, 0.0, x)], axis=0)
        other = jnp.concatenate(
            [jnp.where(first, 0.0, turned_x), jnp.where(first, turned_x, 0.0)], axis=0
        )
        return direct, other

    across = lax.broadcasted_iota(jnp.int32, (run, listed), 1)
    down = lax.broadcasted_iota(jnp.int32, (run, listed), 0)
    move[...] = jnp.concatenate(
        [
            jnp.where(across == down + (part_at * packed + o * run), 1.0, 0.0)
            for o in range(partners)
            for part_at in range(2)
        ],
        axis=0,
    ).astype(BF16)

    def picked(x):
        hi, mid = split2(x)
        low = ((x - hi.astype(F32)) - mid.astype(F32)).astype(BF16)
        wide = dot(pick[...], jnp.concatenate([hi, mid], axis=1))
        return (wide[:, :LANES] + wide[:, LANES:]) + dot(pick[...], low)

    loads[1].wait()
    for half in range(halves):
        groups = pack(picked(v0[:, half * LANES : (half + 1) * LANES]))
        for q in range(2):
            pay[0, 2 * half + q] = groups[q]
            if half == 0 and q == 0:
                pl.semaphore_wait(barrier, partners)
            send(0, 2 * half + q)

    def build(which):
        for g in range(blocks):
            named = [cols[which, g, k] for k in range(slots)]
            for c in range(ext_blocks):
                total = None
                for k in range(slots):
                    term = tiles[which, g, k] * jnp.where(named[k] == c, 1.0, 0.0).astype(F32)
                    total = term if total is None else total + term
                hi, lo = split2(total)
                rows = slice(listed + g * size, listed + (g + 1) * size)
                w_hi[which, rows, c * size : (c + 1) * size] = hi
                w_lo[which, rows, c * size : (c + 1) * size] = lo
        for w, u in ((w_hi, u_hi), (w_lo, u_lo)):
            w[which, listed:, own:] = dot(w[which, listed:, own:], move[...]).astype(BF16)
            top = dot(pick[...], w[which, listed:])
            w[which, 0:listed, 0:own] = top[:, 0:own].astype(BF16)
            one, two = top[0:packed, own:], top[packed:, own:]
            in_one = lax.broadcasted_iota(jnp.int32, (packed, listed), 1) < packed
            u[which, :, 0:listed] = jnp.where(in_one, one, two).astype(BF16)
            u[which, :, listed:] = jnp.where(in_one, two, one).astype(BF16)

    loads[2].wait()
    loads[3].wait()
    build(0)
    loads[4].wait()
    for half in range(halves):
        psrc[half] = picked(src[:, half * LANES : (half + 1) * LANES])

    def source_of(half):
        return src[:, half * LANES : (half + 1) * LANES]

    def settle(half, state, add_source):
        hi, lo = split2(state)
        vcat[half, :, 0:LANES] = hi
        vcat[half, :, LANES:] = lo
        vpart[half] = state + source_of(half) if add_source else state

    def near_head(which, half, exchange, add_source):
        head = product(w_hi[which, 0:listed, 0:own], w_lo[which, 0:listed, 0:own], vcat[half])
        groups = pack(head + psrc[half] if add_source else head)
        for q in range(2):
            part[2 * half + q] = pay[exchange, 2 * half + q] + groups[q]

    def near_body(which, half):
        vpart[half] = vpart[half] + product(
            w_hi[which, listed:, 0:own], w_lo[which, listed:, 0:own], vcat[half]
        )

    for half in range(halves):
        settle(half, v0[:, half * LANES : (half + 1) * LANES], True)
        near_head(0, half, 0, True)
        near_body(0, half)
    loads[5].wait()
    loads[6].wait()
    build(1)

    def urgent(exchange, which, group, last):
        arrived = halo.at[exchange, group]
        pltpu.make_async_copy(arrived, arrived, recv_sem.at[exchange % 2, group]).wait()
        direct, other = [jnp.concatenate(split2(x), axis=1) for x in unpack(arrived[...])]
        if not last:
            both = jnp.concatenate([direct, other], axis=0)
            pay[exchange + 1, group] = part[group] + product(u_hi[which], u_lo[which], both)
            send(exchange + 1, group)
        if group % 2 == 0:
            hcat[...] = jnp.concatenate([direct[0:packed], other[packed:]], axis=0)
        else:
            hcat[...] += jnp.concatenate([other[0:packed], direct[packed:]], axis=0)

    def far_body(which, half):
        return vpart[half] + product(
            w_hi[which, listed:, own:], w_lo[which, listed:, own:], hcat[...]
        )

    waiting = []
    for exchange in range(exchanges):
        which = exchange % 2
        last = exchange == exchanges - 1
        for group in range(2 * halves):
            urgent(exchange, which, group, last)
            if waiting:
                waiting.pop(0)()
            if group % 2 == 1:
                half = group // 2
                state = far_body(which, half)
                if last:
                    out_ref[:, half * LANES : (half + 1) * LANES] = state
                    continue
                settle(half, state, which == 1)
                if exchange + 2 < exchanges:
                    waiting.append(
                        functools.partial(near_head, 1 - which, half, exchange + 1, which == 1)
                    )
                waiting.append(functools.partial(near_body, 1 - which, half))

    for exchange in range(exchanges):
        sent = pay.at[exchange]
        pltpu.make_async_copy(sent, sent, send_sem.at[exchange]).wait()


def on_device(devices, v0, source, et, it, ec, ic, send):
    own, panels = v0.shape
    partners, per_list = send.shape
    blocks, slots, size, _ = et.shape
    listed = partners * per_list
    extended = own + listed
    halves = panels // LANES
    exchanges = 2 * STEPS
    in_hbm = pl.BlockSpec(memory_space=pltpu.HBM)
    return pl.pallas_call(
        functools.partial(kernel, devices),
        out_shape=jax.ShapeDtypeStruct((own, panels), F32),
        in_specs=[in_hbm] * 7,
        out_specs=pl.BlockSpec(memory_space=pltpu.VMEM),
        scratch_shapes=[
            pltpu.VMEM((own, panels), F32),
            pltpu.VMEM((own, panels), F32),
            pltpu.VMEM((2, blocks, slots, size, size), F32),
            pltpu.SMEM((2, blocks, slots), jnp.int32),
            pltpu.VMEM((partners, per_list), jnp.int32),
            pltpu.VMEM((LANES, LANES), F32),
            pltpu.VMEM((listed, own), BF16),
            pltpu.VMEM((listed, listed), BF16),
            pltpu.VMEM((2, extended, extended), BF16),
            pltpu.VMEM((2, extended, extended), BF16),
            pltpu.VMEM((2, listed // 2, 2 * listed), BF16),
            pltpu.VMEM((2, listed // 2, 2 * listed), BF16),
            pltpu.VMEM((exchanges, 2 * halves, listed // 2, LANES), F32),
            pltpu.VMEM((exchanges, 2 * halves, listed // 2, LANES), F32),
            pltpu.VMEM((halves, own, 2 * LANES), BF16),
            pltpu.VMEM((listed, 2 * LANES), BF16),
            pltpu.VMEM((halves, own, LANES), F32),
            pltpu.VMEM((2 * halves, listed // 2, LANES), F32),
            pltpu.VMEM((halves, listed, LANES), F32),
            pltpu.SemaphoreType.DMA((7,)),
            pltpu.SemaphoreType.DMA((exchanges,)),
            pltpu.SemaphoreType.DMA((2, 2 * halves)),
        ],
        compiler_params=pltpu.CompilerParams(
            collective_id=0, has_side_effects=True, vmem_limit_bytes=48 * 1024 * 1024
        ),
    )(
        *[
            pltpu.with_memory_space_constraint(x, pltpu.HBM)
            for x in (v0, source, et, it, ec, ic, send)
        ]
    )


def solution(mesh):
    return jax.shard_map(
        functools.partial(on_device, mesh.shape["rows"]),
        mesh=mesh,
        in_specs=(
            P("rows", None),
            P("rows", None),
            P("rows", None, None, None),
            P("rows", None, None, None),
            P("rows", None),
            P("rows", None),
            P("rows", None),
        ),
        out_specs=P("rows", None),
        check_vma=False,
    )
```
